32 devices in a mesh: rep: 2 (over z, core), dp: 16 (over x, y).
Axes of the slice: x: 4, y: 4, z: 1, core: 2. Of those that a mesh axis runs over, the one named last changes fastest.
The devices are a block of a 4x4x8 slice.
Arguments:
- g_w_gate: bfloat16 [32, 2, 896, 2304], P(('rep', 'dp')), parts along dimension 0
- g_w_up: bfloat16 [32, 2, 896, 2304], P(('rep', 'dp')), parts along dimension 0
- g_w_down: bfloat16 [32, 2, 2304, 896], P(('rep', 'dp')), parts along dimension 0
- w_gate: bfloat16 [2, 896, 2304], replicated
- w_up: bfloat16 [2, 896, 2304], replicated
- w_down: bfloat16 [2, 2304, 896], replicated
- m_w_gate: float32 [2, 896, 2304], P(None, 'dp')
- m_w_up: float32 [2, 896, 2304], P(None, 'dp')
- m_w_down: float32 [2, 2304, 896], P(None, 'dp')
- v_w_gate: float32 [2, 896, 2304], P(None, 'dp')
- v_w_up: float32 [2, 896, 2304], P(None, 'dp')
- v_w_down: float32 [2, 2304, 896], P(None, 'dp')
Outputs:
- output 1: bfloat16 [4, 896, 2304], P('rep'), parts along dimension 0
- output 2: bfloat16 [4, 896, 2304], P('rep'), parts along dimension 0
- output 3: bfloat16 [4, 2304, 896], P('rep'), parts along dimension 0
- output 4: float32 [4, 896, 2304], P('rep', 'dp'), parts along dimension 0
- output 5: float32 [4, 896, 2304], P('rep', 'dp'), parts along dimension 0
- output 6: float32 [4, 2304, 896], P('rep', 'dp'), parts along dimension 0
- output 7: float32 [4, 896, 2304], P('rep', 'dp'), parts along dimension 0
- output 8: float32 [4, 896, 2304], P('rep', 'dp'), parts along dimension 0
- output 9: float32 [4, 2304, 896], P('rep', 'dp'), parts along dimension 0
There are 2 independent parts. The reference program is written for one: setup_inputs(seed, part) draws one part's arguments, and reference() takes and returns one part's arrays. A program takes and returns all parts, laid end to end along the dimension named above; an argument that names none is the same for every part.
All inputs are finite; a program needn't handle non-finite values.
Results may differ from the reference program's by a relative error of at most 0.022.
Values are sent between devices in bfloat16 or wider.
A program may use at most 768 MiB of HBM per device.

```python
import jax
import jax.numpy as jnp
from jax import lax

DEVICES = 16
D = 896
FF = 2304
LAYERS = 2
NAMES = ("w_gate", "w_up", "w_down")
SHAPES = {"w_gate": (LAYERS, D, FF), "w_up": (LAYERS, D, FF), "w_down": (LAYERS, FF, D)}


def setup_inputs(seed: int = 0, part: int = 0) -> dict:
    kz, *keys = jax.random.split(jax.random.key(seed), 1 + 5 * len(NAMES))
    loud = 2.0 ** jax.random.uniform(kz, (), jnp.float32, -1.0, 1.0)
    drawn = {}
    for name, key, both in zip(NAMES, keys[:3], keys[3:6], strict=True):
        own = jax.random.normal(jax.random.fold_in(key, part), (DEVICES, *SHAPES[name]), jnp.float32)
        shared = jax.random.normal(jax.random.fold_in(both, part), SHAPES[name], jnp.float32)
        drawn["g_" + name] = (loud * (0.7 * shared / DEVICES + 0.7 * own * DEVICES**-0.5)).astype(jnp.bfloat16)
    for name, key in zip(NAMES, keys[6:9], strict=True):
        drawn[name] = (jax.random.normal(key, SHAPES[name], jnp.float32) * SHAPES[name][1] ** -0.5).astype(jnp.bfloat16)
    for name, key in zip(NAMES, keys[9:12], strict=True):
        drawn["m_" + name] = loud * 0.5 * jax.random.normal(key, SHAPES[name], jnp.float32)
    for name, key in zip(NAMES, keys[12:15], strict=True):
        drawn["v_" + name] = loud * loud * jax.random.uniform(key, SHAPES[name], jnp.float32, 0.5, 1.5)
    return drawn


def adamw(w, m, v, g):
    m = 0.9 * m + 0.1 * g
    v = 0.95 * v + 0.05 * g * g
    step = m * lax.rsqrt(v + 1e-8) + 0.1 * w
    return (w - 0.02 * step).astype(jnp.bfloat16), m, v


def clipped(gradients, sum_of_squares, count):
    factor = jnp.minimum(1.0, 0.5 * lax.rsqrt(sum_of_squares / count + 1e-30))
    return [g * factor for g in gradients]


def reference(g_w_gate, g_w_up, g_w_down, w_gate, w_up, w_down, m_w_gate, m_w_up, m_w_down, v_w_gate, v_w_up, v_w_down):
    def total(terms):
        return lax.scan(lambda so_far, term: (so_far + term.astype(jnp.float32), None), jnp.zeros(terms.shape[1:], jnp.float32), terms)[0]

    gradients = [total(terms).astype(jnp.bfloat16).astype(jnp.float32) for terms in (g_w_gate, g_w_up, g_w_down)]
    gradients = clipped(gradients, sum(jnp.sum(g * g) for g in gradients), sum(g.size for g in gradients))
    new = [
        adamw(w.astype(jnp.float32), m, v, g)
        for w, m, v, g in zip((w_gate, w_up, w_down), (m_w_gate, m_w_up, m_w_down), (v_w_gate, v_w_up, v_w_down), gradients, strict=True)
    ]
    return tuple(one[which] for which in range(3) for one in new)
```

```python
import functools
import heapq
import math

import jax
import jax.numpy as jnp
from jax import lax
from jax.experimental import pallas as pl
from jax.experimental.pallas import tpu as pltpu
from jax.sharding import PartitionSpec as P

F32, BF16 = jnp.float32, jnp.bfloat16
MESH = pl.DeviceIdType.MESH
SIGN = (1, -1)


def gather_order(side):
    free = {(a, d): 0.0 for a in range(2) for d in range(2)}
    size = (2.0, 1.0)
    events, start, order, count = [], [], [], 0

    def enqueue(now, link, piece, d, first):
        nonlocal count
        c, r1, r2, h, p = piece
        free[link] = max(free[link], now) + size[p]
        there = (c, (r1 - SIGN[d]) % side, r2, h, p) if first else (c, r1, (r2 - SIGN[d]) % side, h, p)
        count += 1
        heapq.heappush(events, (free[link] + 1.0, count, there, link))

    def sends(piece, link):
        c, r1, r2, h, p = piece
        axes = (1, 0) if c == 0 else (0, 1)
        out = []
        if r1 == 0 and r2 == 0:
            out += [(axes[0], d, True) for d in range(2)]
        if r2 == 0:
            if r1 != 0 and r1 != 2 and link[1] == h:
                out.append((axes[0], h, True))
            out += [(axes[1], d, False) for d in range(2)]
        elif r2 != 2 and link[1] == h:
            out.append((axes[1], h, False))
        return out

    now = 0.0
    for p in (1, 0):
        for h in range(2):
            for c in range(2):
                piece = (c, 0, 0, h, p)
                todo = sends(piece, None)
                start.append((piece, todo))
                for a, d, first in todo:
                    enqueue(now, (a, d), piece, d, first)
                now += 0.1
    while events:
        now, _, piece, link = heapq.heappop(events)
        todo = sends(piece, link)
        order.append((piece, todo))
        for a, d, first in todo:
            enqueue(now, (a, d), piece, d, first)
    return start, order


def columns(shape):
    return 384 if shape[-1] % 384 == 0 else 128


def loop(shape, body, carry=0):
    width = columns(shape)

    def step(i, carry):
        return body(pl.ds(pl.multiple_of(i * width, width), width), carry)

    return lax.fori_loop(0, shape[-1] // width, step, carry)


def squares(x):
    total = None
    for i in range(0, x.shape[0], 8):
        for j in range(0, x.shape[1], 128):
            one = x[i : i + 8, j : j + 128]
            total = one * one if total is None else total + one * one
    return total


def kernel(n, side, count, ga, gb, gd, wa, wb, wd, ma, mb, md, va, vb, vd,
           oa, ob, od, oma, omb, omd, ova, ovb, ovd,
           fwd_big, fwd_small, own_big, own_small, acc_big, acc_small, w_big, w_small, part,
           load_sem, send_big, send_small, recv, part_send, part_recv):
    me = lax.axis_index("dp")
    at = (me // side, me % side)

    def block(c, q1, q2):
        return q1 * side + q2 if c == 0 else q2 * side + q1

    def neighbour(axis, d):
        moved = lax.rem(at[axis] + SIGN[d] + side, side)
        return moved * side + at[1] if axis == 0 else at[0] * side + moved

    def near(p, steps):
        return lax.rem(p + steps + side, side)

    g_big, out_big = (ga, gb), (oa, ob)

    loads = {}

    def load(key, index, src, dst):
        copy = pltpu.make_async_copy(src, dst, load_sem.at[index])
        copy.start()
        loads[key] = copy

    def rows(ref, c, q1):
        return ref.at[c, q1] if c == 0 else ref.at[c, :, q1]

    index = 0
    for d in range(2):
        for c in range(2):
            q1 = near(at[c], SIGN[d])
            load(("fwd", c, d, 0), index, rows(g_big[d], c, q1), fwd_big.at[c, d])
            load(("fwd", c, d, 1), index + 1, (gd.at[c, q1, :, d] if c == 0 else gd.at[c, :, q1, d]), fwd_small.at[c, d])
            index += 2
    for h in range(2):
        for c in range(2):
            load(("own", c, h, 0), index, rows(g_big[h], c, at[c]), own_big.at[c, h])
            load(("own", c, h, 1), index + 1, (gd.at[c, at[c], :, h] if c == 0 else gd.at[c, :, at[c], h]), own_small.at[c, h])
            index += 2

    barrier = pltpu.get_barrier_semaphore()
    for i in range(1, n):
        pl.semaphore_signal(barrier, inc=1, device_id={"dp": lax.rem(me + i, n)}, device_id_type=MESH)
    pl.semaphore_wait(barrier, n - 1)

    def slot(c, d, p, s):
        return out_big[d].at[c * n + s] if p == 0 else od.at[c * n + s, d]

    def send(src, dst, axis, d, p, sem):
        sems = send_big if p == 0 else send_small
        link = 2 * axis + d
        pltpu.make_async_remote_copy(
            src_ref=src, dst_ref=dst, send_sem=sems.at[link if p == 0 else axis], recv_sem=sem,
            device_id={"dp": neighbour(axis, d)}, device_id_type=MESH).start()

    def arrived(ref, sem):
        pltpu.make_async_copy(ref, ref, sem).wait()

    def to_slot(src, c, d, axis, p, s):
        send(src, slot(c, d, p, s), axis, d, p, recv.at[c, d, p, s])

    def wait_slot(c, d, p, s):
        arrived(slot(c, d, p, s), recv.at[c, d, p, s])

    def term_ref(c, h, p, q1, q2):
        i, j = (q1, q2) if c == 0 else (q2, q1)
        return g_big[h].at[c, i, j] if p == 0 else gd.at[c, i, j, h]

    ks = (2, 1, -1, 0)

    def step1(c, d, k):
        for p in range(2):
            to_slot(term_ref(c, d, p, near(at[c], 2), near(at[1 - c], ks[k])), c, d, c, p, k)

    def step2(c, d, k):
        for p in range(2):
            to_slot(term_ref(c, 1 - d, p, near(at[c], SIGN[d]), near(at[1 - c], ks[k])), c, d, c, p, 4 + k)

    for k in range(4):
        for d in range(2):
            for c in range(2):
                step1(c, d, k)
    for k in range(2):
        for d in range(2):
            for c in range(2):
                step2(c, d, k)

    own = (own_big, own_small)
    fwd = (fwd_big, fwd_small)
    acc = (acc_big, acc_small)
    shapes = (own_big.shape[-2:], own_small.shape[-2:])

    for copy in list(loads.values())[: 8]:
        copy.wait()

    def add_fwd(c, d, p, s, src):
        dst = slot(c, d, p, s)

        def body(cols, _):
            dst[:, cols] = (dst[:, cols].astype(F32) + src[:, cols].astype(F32)).astype(BF16)
            return 0

        loop(shapes[p], body)

    for k in range(4):
        for d in range(2):
            for c in range(2):
                for p in range(2):
                    wait_slot(c, d, p, k)
                    add_fwd(c, d, p, k, fwd[p].at[c, d, near(at[1 - c], ks[k])])
                    to_slot(slot(c, d, p, k), c, d, c, p, 8 + k)
                if k < 2:
                    step2(c, d, k + 2)

    for copy in list(loads.values())[8:]:
        copy.wait()

    updates = {}
    for h, (m, v, w, om, ov) in enumerate(((ma, va, wa, oma, ova), (mb, vb, wb, omb, ovb))):
        load(("m", h, 0), index, m, om)
        load(("v", h, 0), index + 1, v, ov)
        load(("w", h, 0), index + 2, w.at[:, me], w_big.at[h])
        index += 3
    load(("m", 1), index, md, omd)
    load(("v", 1), index + 1, vd, ovd)
    load(("w", 1), index + 2, wd.at[:, me], w_small)

    for k in range(4):
        for h in range(2):
            for c in range(2):
                q2 = near(at[1 - c], ks[k])
                for p in range(2):
                    wait_slot(c, h, p, 8 + k)
                    wait_slot(c, 1 - h, p, 4 + k)
                    mine, one, two = own[p].at[c, h, q2], slot(c, h, p, 8 + k), slot(c, 1 - h, p, 4 + k)
                    dst = mine if k < 3 else acc[p].at[c, h]

                    def body(cols, _, mine=mine, one=one, two=two, dst=dst):
                        x = mine[:, cols].astype(F32) + one[:, cols].astype(F32) + two[:, cols].astype(F32)
                        dst[:, cols] = x.astype(dst.dtype)
                        return 0

                    loop(shapes[p], body)
                    if k == 0:
                        to_slot(mine, c, h, 1 - c, p, 12)
                    if (k == 1 and h == 1) or (k == 2 and h == 0):
                        to_slot(mine, c, 1 - h, 1 - c, p, 13)

    for p in range(2):
        for d in range(2):
            for c in range(2):
                wait_slot(c, d, p, 12)
                add_fwd(c, d, p, 12, own[p].at[c, d, near(at[1 - c], SIGN[d])])
                to_slot(slot(c, d, p, 12), c, d, 1 - c, p, 14)

    total = jnp.zeros((8, 128), F32)
    for p in range(2):
        for h in range(2):
            for c in range(2):
                wait_slot(c, h, p, 14)
                wait_slot(c, 1 - h, p, 13)
                mine, one, two = acc[p].at[c, h], slot(c, h, p, 14), slot(c, 1 - h, p, 13)

                def body(cols, total, mine=mine, one=one, two=two):
                    x = mine[:, cols] + one[:, cols].astype(F32) + two[:, cols].astype(F32)
                    x = x.astype(BF16).astype(F32)
                    mine[:, cols] = x
                    return total + squares(x)

                total = loop(shapes[p], body, total)

    def wait_sends():
        many = n - 1
        for link in range(4):
            ref = oa.at[pl.ds(0, many)]
            pltpu.make_async_copy(ref, ref, send_big.at[link]).wait()
        for axis in range(2):
            ref = od.at[pl.ds(0, many)]
            pltpu.make_async_copy(ref, ref, send_small.at[axis]).wait()

    wait_sends()

    part[me] = total
    copies = []
    for i in range(1, n):
        to = lax.rem(me + i, n)
        copy = pltpu.make_async_remote_copy(
            src_ref=part.at[me], dst_ref=part.at[me], send_sem=part_send.at[i - 1], recv_sem=part_recv.at[i - 1],
            device_id={"dp": to}, device_id_type=MESH)
        copy.start()
        copies.append(copy)
    for copy in list(loads.values())[16:]:
        copy.wait()
    for i in range(1, n):
        back = lax.rem(me - i + n, n)
        arrived(part.at[back], part_recv.at[i - 1])
    total = part[0]
    for i in range(1, n):
        total = total + part[i]
    total = jnp.sum(total, keepdims=True)
    factor = jnp.minimum(1.0, 0.5 * lax.rsqrt(total / count + 1e-30))

    oms, ovs = (oma, omb), (ova, ovb)
    start, order = gather_order(side)

    def gathered(piece):
        c, r1, r2, h, p = piece
        q1, q2 = near(at[1 - c], r1), near(at[c], r2)
        b = q2 * side + q1 if c == 0 else q1 * side + q2
        return (out_big[h].at[c * n + b] if p == 0 else od.at[c * n + b, h]), recv.at[c, h, p, b]

    def pass_on(piece, todo):
        ref, sem = gathered(piece)
        for a, d, _ in todo:
            send(ref, ref, a, d, piece[-1], sem)

    for piece, todo in start:
        c, _, _, h, p = piece
        g = acc[p].at[c, h]
        m, v = (oms[h].at[c], ovs[h].at[c]) if p == 0 else (omd.at[c, h], ovd.at[c, h])
        w = w_big.at[h, c] if p == 0 else w_small.at[c, h]
        out, _ = gathered(piece)

        def body(cols, _, g=g, m=m, v=v, w=w, out=out):
            x = g[:, cols] * factor
            m1 = 0.9 * m[:, cols] + 0.1 * x
            v1 = 0.95 * v[:, cols] + 0.05 * x * x
            m[:, cols] = m1
            v[:, cols] = v1
            w1 = w[:, cols].astype(F32)
            out[:, cols] = (w1 - 0.02 * (m1 * lax.rsqrt(v1 + 1e-8) + 0.1 * w1)).astype(BF16)
            return 0

        loop(shapes[p], body)
        pass_on(piece, todo)
    for piece, todo in order:
        arrived(*gathered(piece))
        pass_on(piece, todo)
    wait_sends()
    for copy in copies:
        copy.wait_send()


def write_out(*refs):
    sem = refs[-1]
    copies = [pltpu.make_async_copy(refs[i], refs[9 + i], sem.at[i]) for i in range(9)]
    for copy in copies:
        copy.start()
    for copy in copies:
        copy.wait()


def solution(mesh):
    n = mesh.shape["dp"]
    side = math.isqrt(n)

    def step(*arrays):
        terms, weights, m, v = (arrays[i : i + 3] for i in (0, 3, 6, 9))
        layers, block_rows, wide = m[0].shape
        down_rows, narrow = m[2].shape[1] // 2, m[2].shape[2]
        big, small = (block_rows, wide), (down_rows, narrow)
        ins = [terms[0].reshape(layers, side, side, *big), terms[1].reshape(layers, side, side, *big),
               terms[2].reshape(layers, side, side, 2, *small),
               weights[0].reshape(layers, n, *big), weights[1].reshape(layers, n, *big), weights[2].reshape(layers, n, 2, *small)]
        for three in (m, v):
            ins += [three[0], three[1], three[2].reshape(layers, 2, *small)]
        outs = [((layers * n, *big), BF16)] * 2 + [((layers * n, 2, *small), BF16)]
        outs += ([((layers, *big), F32)] * 2 + [((layers, 2, *small), F32)]) * 2
        count = n * sum(one.size for one in m)
        res = pl.pallas_call(
            functools.partial(kernel, n, side, count),
            out_shape=[pltpu.VMEM(*one) for one in outs],
            in_specs=[pl.BlockSpec(memory_space=pl.ANY)] * 12,
            out_specs=[pl.BlockSpec(memory_space=pltpu.VMEM)] * 9,
            scratch_shapes=[
                pltpu.VMEM((layers, 2, side, *big), BF16),
                pltpu.VMEM((layers, 2, side, *small), BF16),
                pltpu.VMEM((layers, 2, side, *big), BF16),
                pltpu.VMEM((layers, 2, side, *small), BF16),
                pltpu.VMEM((layers, 2, *big), F32),
                pltpu.VMEM((layers, 2, *small), F32),
                pltpu.VMEM((2, layers, *big), BF16),
                pltpu.VMEM((layers, 2, *small), BF16),
                pltpu.VMEM((n, 8, 128), F32),
                pltpu.SemaphoreType.DMA((25,)),
                pltpu.SemaphoreType.DMA((4,)),
                pltpu.SemaphoreType.DMA((2,)),
                pltpu.SemaphoreType.DMA((layers, 2, 2, n)),
                pltpu.SemaphoreType.DMA((n - 1,)),
                pltpu.SemaphoreType.DMA((n - 1,)),
            ],
            compiler_params=pltpu.CompilerParams(collective_id=0, has_side_effects=True, vmem_limit_bytes=24 * 2**20),
        )(*ins)
        res = pl.pallas_call(
            write_out,
            out_shape=[jax.ShapeDtypeStruct(*one) for one in outs],
            in_specs=[pl.BlockSpec(memory_space=pltpu.VMEM)] * 9,
            out_specs=[pl.BlockSpec(memory_space=pl.ANY)] * 9,
            scratch_shapes=[pltpu.SemaphoreType.DMA((9,))],
            compiler_params=pltpu.CompilerParams(vmem_limit_bytes=2**20),
        )(*res)
        return tuple(r.reshape(layers, -1, r.shape[-1]) for r in res)

    all_of, cut = P(None, None, None), P(None, "dp", None)
    return jax.shard_map(
        step,
        mesh=mesh,
        in_specs=(P(("rep", "dp"), None, None, None),) * 3 + (all_of,) * 3 + (cut,) * 6,
        out_specs=(P("rep", None, None),) * 3 + (P("rep", "dp", None),) * 6,
        check_vma=False,
    )
```

```python
import functools
import heapq
import math

import jax
import jax.numpy as jnp
from jax import lax
from jax.experimental import pallas as pl
from jax.experimental.pallas import tpu as pltpu
from jax.sharding import PartitionSpec as P

F32, BF16 = jnp.float32, jnp.bfloat16
MESH = pl.DeviceIdType.MESH
SIGN = (1, -1)


def gather_order(side):
    free = {(a, d): 0.0 for a in range(2) for d in range(2)}
    size = (2.0, 1.0)
    events, start, order, count = [], [], [], 0

    def enqueue(now, link, piece, d, first):
        nonlocal count
        c, r1, r2, h, p = piece
        free[link] = max(free[link], now) + size[p]
        there = (c, (r1 - SIGN[d]) % side, r2, h, p) if first else (c, r1, (r2 - SIGN[d]) % side, h, p)
        count += 1
        heapq.heappush(events, (free[link] + 1.0, count, there, link))

    def sends(piece, link):
        c, r1, r2, h, p = piece
        axes = (1, 0) if c == 0 else (0, 1)
        out = []
        if r1 == 0 and r2 == 0:
            out += [(axes[0], d, True) for d in range(2)]
        if r2 == 0:
            if r1 != 0 and r1 != 2 and link[1] == h:
                out.append((axes[0], h, True))
            out += [(axes[1], d, False) for d in range(2)]
        elif r2 != 2 and link[1] == h:
            out.append((axes[1], h, False))
        return out

    now = 0.0
    for p in (1, 0):
        for h in range(2):
            for c in range(2):
                piece = (c, 0, 0, h, p)
                todo = sends(piece, None)
                start.append((piece, todo))
                for a, d, first in todo:
                    enqueue(now, (a, d), piece, d, first)
                now += 0.1
    while events:
        now, _, piece, link = heapq.heappop(events)
        todo = sends(piece, link)
        order.append((piece, todo))
        for a, d, first in todo:
            enqueue(now, (a, d), piece, d, first)
    return start, order


def columns(shape):
    return 384 if shape[-1] % 384 == 0 else 128


def loop(shape, body, carry=0):
    width = columns(shape)

    def step(i, carry):
        return body(pl.ds(pl.multiple_of(i * width, width), width), carry)

    return lax.fori_loop(0, shape[-1] // width, step, carry)


def squares(x):
    total = None
    for i in range(0, x.shape[0], 8):
        for j in range(0, x.shape[1], 128):
            one = x[i : i + 8, j : j + 128]
            total = one * one if total is None else total + one * one
    return total


def kernel(n, side, count, ga, gb, gd, wa, wb, wd, ma, mb, md, va, vb, vd,
           oa, ob, od, oma, omb, omd, ova, ovb, ovd,
           fwd_big, fwd_small, own_big, own_small, acc_big, acc_small, w_big, w_small, part,
           load_sem, send_big, send_small, recv, part_send, part_recv):
    me = lax.axis_index("dp")
    at = (me // side, me % side)

    def block(c, q1, q2):
        return q1 * side + q2 if c == 0 else q2 * side + q1

    def neighbour(axis, d):
        moved = lax.rem(at[axis] + SIGN[d] + side, side)
        return moved * side + at[1] if axis == 0 else at[0] * side + moved

    def near(p, steps):
        return lax.rem(p + steps + side, side)

    g_big, out_big = (ga, gb), (oa, ob)

    loads = {}

    def load(key, index, src, dst):
        copy = pltpu.make_async_copy(src, dst, load_sem.at[index])
        copy.start()
        loads[key] = copy

    def rows(ref, c, q1):
        return ref.at[c, q1] if c == 0 else ref.at[c, :, q1]

    barrier = pltpu.get_barrier_semaphore()
    for axis in range(2):
        for d in range(2):
            pl.semaphore_signal(barrier, inc=1, device_id={"dp": neighbour(axis, d)}, device_id_type=MESH)
    pl.semaphore_wait(barrier, 4)

    def slot(c, d, p, s):
        return out_big[d].at[c * n + s] if p == 0 else od.at[c * n + s, d]

    def send(src, dst, axis, d, p, sem):
        sems = send_big if p == 0 else send_small
        link = 2 * axis + d
        pltpu.make_async_remote_copy(
            src_ref=src, dst_ref=dst, send_sem=sems.at[link if p == 0 else axis], recv_sem=sem,
            device_id={"dp": neighbour(axis, d)}, device_id_type=MESH).start()

    def arrived(ref, sem):
        pltpu.make_async_copy(ref, ref, sem).wait()

    def to_slot(src, c, d, axis, p, s):
        send(src, slot(c, d, p, s), axis, d, p, recv.at[c, d, p, s])

    def wait_slot(c, d, p, s):
        arrived(slot(c, d, p, s), recv.at[c, d, p, s])

    def term_ref(c, h, p, q1, q2):
        i, j = (q1, q2) if c == 0 else (q2, q1)
        return g_big[h].at[c, i, j] if p == 0 else gd.at[c, i, j, h]

    ks = (2, 1, -1, 0)

    def step1(c, d, k):
        for p in range(2):
            to_slot(term_ref(c, d, p, near(at[c], 2), near(at[1 - c], ks[k])), c, d, c, p, k)

    def step2(c, d, k):
        for p in range(2):
            to_slot(term_ref(c, 1 - d, p, near(at[c], SIGN[d]), near(at[1 - c], ks[k])), c, d, c, p, 4 + k)

    for k in range(4):
        for d in range(2):
            for c in range(2):
                step1(c, d, k)
    for k in range(2):
        for d in range(2):
            for c in range(2):
                step2(c, d, k)

    index = 0
    for d in range(2):
        for c in range(2):
            q1 = near(at[c], SIGN[d])
            load(("fwd", c, d, 0), index, rows(g_big[d], c, q1), fwd_big.at[c, d])
            load(("fwd", c, d, 1), index + 1, (gd.at[c, q1, :, d] if c == 0 else gd.at[c, :, q1, d]), fwd_small.at[c, d])
            index += 2
    for h in range(2):
        for c in range(2):
            load(("own", c, h, 0), index, rows(g_big[h], c, at[c]), own_big.at[c, h])
            load(("own", c, h, 1), index + 1, (gd.at[c, at[c], :, h] if c == 0 else gd.at[c, :, at[c], h]), own_small.at[c, h])
            index += 2

    own = (own_big, own_small)
    fwd = (fwd_big, fwd_small)
    acc = (acc_big, acc_small)
    shapes = (own_big.shape[-2:], own_small.shape[-2:])

    for copy in list(loads.values())[: 8]:
        copy.wait()

    def add_fwd(c, d, p, s, src):
        dst = slot(c, d, p, s)

        def body(cols, _):
            dst[:, cols] = (dst[:, cols].astype(F32) + src[:, cols].astype(F32)).astype(BF16)
            return 0

        loop(shapes[p], body)

    for k in range(4):
        for d in range(2):
            for c in range(2):
                for p in range(2):
                    wait_slot(c, d, p, k)
                    add_fwd(c, d, p, k, fwd[p].at[c, d, near(at[1 - c], ks[k])])
                    to_slot(slot(c, d, p, k), c, d, c, p, 8 + k)
                if k < 2:
                    step2(c, d, k + 2)

    for copy in list(loads.values())[8:]:
        copy.wait()

    updates = {}
    for h, (m, v, w, om, ov) in enumerate(((ma, va, wa, oma, ova), (mb, vb, wb, omb, ovb))):
        load(("m", h, 0), index, m, om)
        load(("v", h, 0), index + 1, v, ov)
        load(("w", h, 0), index + 2, w.at[:, me], w_big.at[h])
        index += 3
    load(("m", 1), index, md, omd)
    load(("v", 1), index + 1, vd, ovd)
    load(("w", 1), index + 2, wd.at[:, me], w_small)

    for k in range(4):
        for h in range(2):
            for c in range(2):
                q2 = near(at[1 - c], ks[k])
                for p in range(2):
                    wait_slot(c, h, p, 8 + k)
                    wait_slot(c, 1 - h, p, 4 + k)
                    mine, one, two = own[p].at[c, h, q2], slot(c, h, p, 8 + k), slot(c, 1 - h, p, 4 + k)
                    dst = mine if k < 3 else acc[p].at[c, h]

                    def body(cols, _, mine=mine, one=one, two=two, dst=dst):
                        x = mine[:, cols].astype(F32) + one[:, cols].astype(F32) + two[:, cols].astype(F32)
                        dst[:, cols] = x.astype(dst.dtype)
                        return 0

                    loop(shapes[p], body)
                    if k == 0:
                        to_slot(mine, c, h, 1 - c, p, 12)
                    if (k == 1 and h == 1) or (k == 2 and h == 0):
                        to_slot(mine, c, 1 - h, 1 - c, p, 13)

    for p in range(2):
        for d in range(2):
            for c in range(2):
                wait_slot(c, d, p, 12)
                add_fwd(c, d, p, 12, own[p].at[c, d, near(at[1 - c], SIGN[d])])
                to_slot(slot(c, d, p, 12), c, d, 1 - c, p, 14)

    total = jnp.zeros((8, 128), F32)
    for p in range(2):
        for h in range(2):
            for c in range(2):
                wait_slot(c, h, p, 14)
                wait_slot(c, 1 - h, p, 13)
                mine, one, two = acc[p].at[c, h], slot(c, h, p, 14), slot(c, 1 - h, p, 13)

                def body(cols, total, mine=mine, one=one, two=two):
                    x = mine[:, cols] + one[:, cols].astype(F32) + two[:, cols].astype(F32)
                    x = x.astype(BF16).astype(F32)
                    mine[:, cols] = x
                    return total + squares(x)

                total = loop(shapes[p], body, total)

    def wait_sends():
        many = n - 1
        for link in range(4):
            ref = oa.at[pl.ds(0, many)]
            pltpu.make_async_copy(ref, ref, send_big.at[link]).wait()
        for axis in range(2):
            ref = od.at[pl.ds(0, many)]
            pltpu.make_async_copy(ref, ref, send_small.at[axis]).wait()

    wait_sends()

    part[me] = jnp.sum(total, axis=0, keepdims=True)
    copies = []
    def far(i):
        return sum(min(k, side - k) for k in (i // side, i % side))

    def shifted(i, sign):
        return near(at[0], sign * (i // side)) * side + near(at[1], sign * (i % side))

    for i in sorted(range(1, n), key=far, reverse=True):
        to = shifted(i, 1)
        copy = pltpu.make_async_remote_copy(
            src_ref=part.at[me], dst_ref=part.at[me], send_sem=part_send.at[i - 1], recv_sem=part_recv.at[i - 1],
            device_id={"dp": to}, device_id_type=MESH)
        copy.start()
        copies.append(copy)
    for copy in list(loads.values())[16:]:
        copy.wait()
    for i in range(1, n):
        back = shifted(i, -1)
        arrived(part.at[back], part_recv.at[i - 1])
    total = part[0]
    for i in range(1, n):
        total = total + part[i]
    total = jnp.sum(total, keepdims=True)
    factor = jnp.minimum(1.0, 0.5 * lax.rsqrt(total / count + 1e-30))

    oms, ovs = (oma, omb), (ova, ovb)
    start, order = gather_order(side)

    def gathered(piece):
        c, r1, r2, h, p = piece
        q1, q2 = near(at[1 - c], r1), near(at[c], r2)
        b = q2 * side + q1 if c == 0 else q1 * side + q2
        return (out_big[h].at[c * n + b] if p == 0 else od.at[c * n + b, h]), recv.at[c, h, p, b]

    def pass_on(piece, todo):
        ref, sem = gathered(piece)
        for a, d, _ in todo:
            send(ref, ref, a, d, piece[-1], sem)

    for piece, todo in start:
        c, _, _, h, p = piece
        g = acc[p].at[c, h]
        m, v = (oms[h].at[c], ovs[h].at[c]) if p == 0 else (omd.at[c, h], ovd.at[c, h])
        w = w_big.at[h, c] if p == 0 else w_small.at[c, h]
        out, _ = gathered(piece)

        def body(cols, _, g=g, m=m, v=v, w=w, out=out):
            x = g[:, cols] * factor
            m1 = 0.9 * m[:, cols] + 0.1 * x
            v1 = 0.95 * v[:, cols] + 0.05 * x * x
            m[:, cols] = m1
            v[:, cols] = v1
            w1 = w[:, cols].astype(F32)
            out[:, cols] = (w1 - 0.02 * (m1 * lax.rsqrt(v1 + 1e-8) + 0.1 * w1)).astype(BF16)
            return 0

        loop(shapes[p], body)
        pass_on(piece, todo)
    for piece, todo in order:
        arrived(*gathered(piece))
        pass_on(piece, todo)
    wait_sends()
    for copy in copies:
        copy.wait_send()


def write_out(*refs):
    many = len(refs) // 2
    copies = [pltpu.make_async_copy(refs[i], refs[many + i], refs[-1].at[i]) for i in range(many)]
    for copy in copies:
        copy.start()
    for copy in copies:
        copy.wait()


def solution(mesh):
    n = mesh.shape["dp"]
    side = math.isqrt(n)

    def step(*arrays):
        terms, weights, m, v = (arrays[i : i + 3] for i in (0, 3, 6, 9))
        layers, block_rows, wide = m[0].shape
        down_rows, narrow = m[2].shape[1] // 2, m[2].shape[2]
        big, small = (block_rows, wide), (down_rows, narrow)
        ins = [terms[0].reshape(layers, side, side, *big), terms[1].reshape(layers, side, side, *big),
               terms[2].reshape(layers, side, side, 2, *small),
               weights[0].reshape(layers, n, *big), weights[1].reshape(layers, n, *big), weights[2].reshape(layers, n, 2, *small)]
        for three in (m, v):
            ins += [three[0], three[1], three[2].reshape(layers, 2, *small)]
        outs = [((layers * n, *big), BF16)] * 2 + [((layers * n, 2, *small), BF16)]
        outs += ([((layers, *big), F32)] * 2 + [((layers, 2, *small), F32)]) * 2
        count = n * sum(one.size for one in m)
        res = pl.pallas_call(
            functools.partial(kernel, n, side, count),
            out_shape=[pltpu.VMEM(*one) for one in outs],
            in_specs=[pl.BlockSpec(memory_space=pl.ANY)] * 12,
            out_specs=[pl.BlockSpec(memory_space=pltpu.VMEM)] * 9,
            scratch_shapes=[
                pltpu.VMEM((layers, 2, side, *big), BF16),
                pltpu.VMEM((layers, 2, side, *small), BF16),
                pltpu.VMEM((layers, 2, side, *big), BF16),
                pltpu.VMEM((layers, 2, side, *small), BF16),
                pltpu.VMEM((layers, 2, *big), F32),
                pltpu.VMEM((layers, 2, *small), F32),
                pltpu.VMEM((2, layers, *big), BF16),
                pltpu.VMEM((layers, 2, *small), BF16),
                pltpu.VMEM((n, 1, 128), F32),
                pltpu.SemaphoreType.DMA((25,)),
                pltpu.SemaphoreType.DMA((4,)),
                pltpu.SemaphoreType.DMA((2,)),
                pltpu.SemaphoreType.DMA((layers, 2, 2, n)),
                pltpu.SemaphoreType.DMA((n - 1,)),
                pltpu.SemaphoreType.DMA((n - 1,)),
            ],
            compiler_params=pltpu.CompilerParams(collective_id=0, has_side_effects=True, vmem_limit_bytes=24 * 2**20),
        )(*ins)
        res = pl.pallas_call(
            write_out,
            out_shape=[jax.ShapeDtypeStruct(*one) for one in outs],
            in_specs=[pl.BlockSpec(memory_space=pltpu.VMEM)] * 9,
            out_specs=[pl.BlockSpec(memory_space=pl.ANY)] * 9,
            scratch_shapes=[pltpu.SemaphoreType.DMA((9,))],
            compiler_params=pltpu.CompilerParams(vmem_limit_bytes=2**20),
        )(*res)
        return tuple(r.reshape(layers, -1, r.shape[-1]) for r in res)

    all_of, cut = P(None, None, None), P(None, "dp", None)
    return jax.shard_map(
        step,
        mesh=mesh,
        in_specs=(P(("rep", "dp"), None, None, None),) * 3 + (all_of,) * 3 + (cut,) * 6,
        out_specs=(P("rep", None, None),) * 3 + (P("rep", "dp", None),) * 6,
        check_vma=False,
    )
```

```python
import functools
import heapq
import math

import jax
import jax.numpy as jnp
from jax import lax
from jax.experimental import pallas as pl
from jax.experimental.pallas import tpu as pltpu
from jax.sharding import PartitionSpec as P

F32, BF16 = jnp.float32, jnp.bfloat16
MESH = pl.DeviceIdType.MESH
SIGN = (1, -1)


def gather_order(side):
    free = {(a, d): 0.0 for a in range(2) for d in range(2)}
    size = (2.0, 1.0)
    events, start, order, count = [], [], [], 0

    def enqueue(now, link, piece, d, first):
        nonlocal count
        c, r1, r2, h, p = piece
        free[link] = max(free[link], now) + size[p]
        there = (c, (r1 - SIGN[d]) % side, r2, h, p) if first else (c, r1, (r2 - SIGN[d]) % side, h, p)
        count += 1
        heapq.heappush(events, (free[link] + 1.0, count, there, link))

    def sends(piece, link):
        c, r1, r2, h, p = piece
        axes = (1, 0) if c == 0 else (0, 1)
        out = []
        if r1 == 0 and r2 == 0:
            out += [(axes[0], d, True) for d in range(2)]
        if r2 == 0:
            if r1 != 0 and r1 != 2 and link[1] == h:
                out.append((axes[0], h, True))
            out += [(axes[1], d, False) for d in range(2)]
        elif r2 != 2 and link[1] == h:
            out.append((axes[1], h, False))
        return out

    now = 0.0
    for p in (1, 0):
        for h in range(2):
            for c in range(2):
                piece = (c, 0, 0, h, p)
                todo = sends(piece, None)
                start.append((piece, todo))
                for a, d, first in todo:
                    enqueue(now, (a, d), piece, d, first)
                now += 0.1
    while events:
        now, _, piece, link = heapq.heappop(events)
        todo = sends(piece, link)
        order.append((piece, todo))
        for a, d, first in todo:
            enqueue(now, (a, d), piece, d, first)
    return start, order


def columns(shape):
    return 384 if shape[-1] % 384 == 0 else 128


def loop(shape, body, carry=0):
    width = columns(shape)

    def step(i, carry):
        return body(pl.ds(pl.multiple_of(i * width, width), width), carry)

    return lax.fori_loop(0, shape[-1] // width, step, carry)


def squares(x):
    total = None
    for i in range(0, x.shape[0], 8):
        for j in range(0, x.shape[1], 128):
            one = x[i : i + 8, j : j + 128]
            total = one * one if total is None else total + one * one
    return total


def kernel(n, side, count, ga, gb, gd, wa, wb, wd, ma, mb, md, va, vb, vd,
           oa, ob, od, oma, omb, omd, ova, ovb, ovd,
           fwd_big, fwd_small, own_big, own_small, acc_big, acc_small, w_big, w_small, part,
           load_sem, send_big, send_small, recv, part_send, part_recv):
    me = lax.axis_index("dp")
    at = (me // side, me % side)

    def block(c, q1, q2):
        return q1 * side + q2 if c == 0 else q2 * side + q1

    def neighbour(axis, d):
        moved = lax.rem(at[axis] + SIGN[d] + side, side)
        return moved * side + at[1] if axis == 0 else at[0] * side + moved

    def near(p, steps):
        return lax.rem(p + steps + side, side)

    g_big, out_big = (ga, gb), (oa, ob)

    loads = {}

    def load(key, index, src, dst):
        copy = pltpu.make_async_copy(src, dst, load_sem.at[index])
        copy.start()
        loads[key] = copy

    def rows(ref, c, q1):
        return ref.at[c, q1] if c == 0 else ref.at[c, :, q1]

    barrier = pltpu.get_barrier_semaphore()
    for axis in range(2):
        for d in range(2):
            pl.semaphore_signal(barrier, inc=1, device_id={"dp": neighbour(axis, d)}, device_id_type=MESH)
    pl.semaphore_wait(barrier, 4)

    @pl.when(lax.rem(lax.axis_index("rep"), 2) == 0)
    def _():
        pl.delay(8000)

    def slot(c, d, p, s):
        return out_big[d].at[c * n + s] if p == 0 else od.at[c * n + s, d]

    def send(src, dst, axis, d, p, sem):
        sems = send_big if p == 0 else send_small
        link = 2 * axis + d
        pltpu.make_async_remote_copy(
            src_ref=src, dst_ref=dst, send_sem=sems.at[link if p == 0 else axis], recv_sem=sem,
            device_id={"dp": neighbour(axis, d)}, device_id_type=MESH).start()

    def arrived(ref, sem):
        pltpu.make_async_copy(ref, ref, sem).wait()

    def to_slot(src, c, d, axis, p, s):
        send(src, slot(c, d, p, s), axis, d, p, recv.at[c, d, p, s])

    def wait_slot(c, d, p, s):
        arrived(slot(c, d, p, s), recv.at[c, d, p, s])

    def term_ref(c, h, p, q1, q2):
        i, j = (q1, q2) if c == 0 else (q2, q1)
        return g_big[h].at[c, i, j] if p == 0 else gd.at[c, i, j, h]

    ks = (2, 1, -1, 0)

    def step1(c, d, k):
        for p in range(2):
            to_slot(term_ref(c, d, p, near(at[c], 2), near(at[1 - c], ks[k])), c, d, c, p, k)

    def step2(c, d, k):
        for p in range(2):
            to_slot(term_ref(c, 1 - d, p, near(at[c], SIGN[d]), near(at[1 - c], ks[k])), c, d, c, p, 4 + k)

    for k in range(4):
        for d in range(2):
            for c in range(2):
                step1(c, d, k)
    for k in range(2):
        for d in range(2):
            for c in range(2):
                step2(c, d, k)

    index = 0
    for d in range(2):
        for c in range(2):
            q1 = near(at[c], SIGN[d])
            load(("fwd", c, d, 0), index, rows(g_big[d], c, q1), fwd_big.at[c, d])
            load(("fwd", c, d, 1), index + 1, (gd.at[c, q1, :, d] if c == 0 else gd.at[c, :, q1, d]), fwd_small.at[c, d])
            index += 2
    for h in range(2):
        for c in range(2):
            load(("own", c, h, 0), index, rows(g_big[h], c, at[c]), own_big.at[c, h])
            load(("own", c, h, 1), index + 1, (gd.at[c, at[c], :, h] if c == 0 else gd.at[c, :, at[c], h]), own_small.at[c, h])
            index += 2

    own = (own_big, own_small)
    fwd = (fwd_big, fwd_small)
    acc = (acc_big, acc_small)
    shapes = (own_big.shape[-2:], own_small.shape[-2:])

    for copy in list(loads.values())[: 8]:
        copy.wait()

    def add_fwd(c, d, p, s, src):
        dst = slot(c, d, p, s)

        def body(cols, _):
            dst[:, cols] = (dst[:, cols].astype(F32) + src[:, cols].astype(F32)).astype(BF16)
            return 0

        loop(shapes[p], body)

    for k in range(4):
        for d in range(2):
            for c in range(2):
                for p in range(2):
                    wait_slot(c, d, p, k)
                    add_fwd(c, d, p, k, fwd[p].at[c, d, near(at[1 - c], ks[k])])
                    to_slot(slot(c, d, p, k), c, d, c, p, 8 + k)
                if k < 2:
                    step2(c, d, k + 2)

    for copy in list(loads.values())[8:]:
        copy.wait()

    updates = {}
    for h, (m, v, w, om, ov) in enumerate(((ma, va, wa, oma, ova), (mb, vb, wb, omb, ovb))):
        load(("m", h, 0), index, m, om)
        load(("v", h, 0), index + 1, v, ov)
        load(("w", h, 0), index + 2, w.at[:, me], w_big.at[h])
        index += 3
    load(("m", 1), index, md, omd)
    load(("v", 1), index + 1, vd, ovd)
    load(("w", 1), index + 2, wd.at[:, me], w_small)

    for k in range(4):
        for h in range(2):
            for c in range(2):
                q2 = near(at[1 - c], ks[k])
                for p in range(2):
                    wait_slot(c, h, p, 8 + k)
                    wait_slot(c, 1 - h, p, 4 + k)
                    mine, one, two = own[p].at[c, h, q2], slot(c, h, p, 8 + k), slot(c, 1 - h, p, 4 + k)
                    dst = mine if k < 3 else acc[p].at[c, h]

                    def body(cols, _, mine=mine, one=one, two=two, dst=dst):
                        x = mine[:, cols].astype(F32) + one[:, cols].astype(F32) + two[:, cols].astype(F32)
                        dst[:, cols] = x.astype(dst.dtype)
                        return 0

                    loop(shapes[p], body)
                    if k == 0:
                        to_slot(mine, c, h, 1 - c, p, 12)
                    if (k == 1 and h == 1) or (k == 2 and h == 0):
                        to_slot(mine, c, 1 - h, 1 - c, p, 13)

    for p in range(2):
        for d in range(2):
            for c in range(2):
                wait_slot(c, d, p, 12)
                add_fwd(c, d, p, 12, own[p].at[c, d, near(at[1 - c], SIGN[d])])
                to_slot(slot(c, d, p, 12), c, d, 1 - c, p, 14)

    total = jnp.zeros((8, 128), F32)
    for p in range(2):
        for h in range(2):
            for c in range(2):
                wait_slot(c, h, p, 14)
                wait_slot(c, 1 - h, p, 13)
                mine, one, two = acc[p].at[c, h], slot(c, h, p, 14), slot(c, 1 - h, p, 13)

                def body(cols, total, mine=mine, one=one, two=two):
                    x = mine[:, cols] + one[:, cols].astype(F32) + two[:, cols].astype(F32)
                    x = x.astype(BF16).astype(F32)
                    mine[:, cols] = x
                    return total + squares(x)

                total = loop(shapes[p], body, total)

    def wait_sends():
        many = n - 1
        for link in range(4):
            ref = oa.at[pl.ds(0, many)]
            pltpu.make_async_copy(ref, ref, send_big.at[link]).wait()
        for axis in range(2):
            ref = od.at[pl.ds(0, many)]
            pltpu.make_async_copy(ref, ref, send_small.at[axis]).wait()

    wait_sends()

    part[me] = jnp.sum(total, axis=0, keepdims=True)
    copies = []
    def far(i):
        return sum(min(k, side - k) for k in (i // side, i % side))

    def shifted(i, sign):
        return near(at[0], sign * (i // side)) * side + near(at[1], sign * (i % side))

    for i in sorted(range(1, n), key=far, reverse=True):
        to = shifted(i, 1)
        copy = pltpu.make_async_remote_copy(
            src_ref=part.at[me], dst_ref=part.at[me], send_sem=part_send.at[i - 1], recv_sem=part_recv.at[i - 1],
            device_id={"dp": to}, device_id_type=MESH)
        copy.start()
        copies.append(copy)
    for copy in list(loads.values())[16:]:
        copy.wait()
    for i in range(1, n):
        back = shifted(i, -1)
        arrived(part.at[back], part_recv.at[i - 1])
    total = part[0]
    for i in range(1, n):
        total = total + part[i]
    total = jnp.sum(total, keepdims=True)
    factor = jnp.minimum(1.0, 0.5 * lax.rsqrt(total / count + 1e-30))

    oms, ovs = (oma, omb), (ova, ovb)
    start, order = gather_order(side)

    def gathered(piece):
        c, r1, r2, h, p = piece
        q1, q2 = near(at[1 - c], r1), near(at[c], r2)
        b = q2 * side + q1 if c == 0 else q1 * side + q2
        return (out_big[h].at[c * n + b] if p == 0 else od.at[c * n + b, h]), recv.at[c, h, p, b]

    def pass_on(piece, todo):
        ref, sem = gathered(piece)
        for a, d, _ in todo:
            send(ref, ref, a, d, piece[-1], sem)

    for piece, todo in start:
        c, _, _, h, p = piece
        g = acc[p].at[c, h]
        m, v = (oms[h].at[c], ovs[h].at[c]) if p == 0 else (omd.at[c, h], ovd.at[c, h])
        w = w_big.at[h, c] if p == 0 else w_small.at[c, h]
        out, _ = gathered(piece)

        def body(cols, _, g=g, m=m, v=v, w=w, out=out):
            x = g[:, cols] * factor
            m1 = 0.9 * m[:, cols] + 0.1 * x
            v1 = 0.95 * v[:, cols] + 0.05 * x * x
            m[:, cols] = m1
            v[:, cols] = v1
            w1 = w[:, cols].astype(F32)
            out[:, cols] = (w1 - 0.02 * (m1 * lax.rsqrt(v1 + 1e-8) + 0.1 * w1)).astype(BF16)
            return 0

        loop(shapes[p], body)
        pass_on(piece, todo)
    for piece, todo in order:
        arrived(*gathered(piece))
        pass_on(piece, todo)
    wait_sends()
    for copy in copies:
        copy.wait_send()


def write_out(*refs):
    many = len(refs) // 2
    copies = [pltpu.make_async_copy(refs[i], refs[many + i], refs[-1].at[i]) for i in range(many)]
    for copy in copies:
        copy.start()
    for copy in copies:
        copy.wait()


def solution(mesh):
    n = mesh.shape["dp"]
    side = math.isqrt(n)

    def step(*arrays):
        terms, weights, m, v = (arrays[i : i + 3] for i in (0, 3, 6, 9))
        layers, block_rows, wide = m[0].shape
        down_rows, narrow = m[2].shape[1] // 2, m[2].shape[2]
        big, small = (block_rows, wide), (down_rows, narrow)
        ins = [terms[0].reshape(layers, side, side, *big), terms[1].reshape(layers, side, side, *big),
               terms[2].reshape(layers, side, side, 2, *small),
               weights[0].reshape(layers, n, *big), weights[1].reshape(layers, n, *big), weights[2].reshape(layers, n, 2, *small)]
        for three in (m, v):
            ins += [three[0], three[1], three[2].reshape(layers, 2, *small)]
        outs = [((layers * n, *big), BF16)] * 2 + [((layers * n, 2, *small), BF16)]
        outs += ([((layers, *big), F32)] * 2 + [((layers, 2, *small), F32)]) * 2
        count = n * sum(one.size for one in m)
        res = pl.pallas_call(
            functools.partial(kernel, n, side, count),
            out_shape=[pltpu.VMEM(*one) for one in outs],
            in_specs=[pl.BlockSpec(memory_space=pl.ANY)] * 12,
            out_specs=[pl.BlockSpec(memory_space=pltpu.VMEM)] * 9,
            scratch_shapes=[
                pltpu.VMEM((layers, 2, side, *big), BF16),
                pltpu.VMEM((layers, 2, side, *small), BF16),
                pltpu.VMEM((layers, 2, side, *big), BF16),
                pltpu.VMEM((layers, 2, side, *small), BF16),
                pltpu.VMEM((layers, 2, *big), F32),
                pltpu.VMEM((layers, 2, *small), F32),
                pltpu.VMEM((2, layers, *big), BF16),
                pltpu.VMEM((layers, 2, *small), BF16),
                pltpu.VMEM((n, 1, 128), F32),
                pltpu.SemaphoreType.DMA((25,)),
                pltpu.SemaphoreType.DMA((4,)),
                pltpu.SemaphoreType.DMA((2,)),
                pltpu.SemaphoreType.DMA((layers, 2, 2, n)),
                pltpu.SemaphoreType.DMA((n - 1,)),
                pltpu.SemaphoreType.DMA((n - 1,)),
            ],
            compiler_params=pltpu.CompilerParams(collective_id=0, has_side_effects=True, vmem_limit_bytes=24 * 2**20),
        )(*ins)
        res = pl.pallas_call(
            write_out,
            out_shape=[jax.ShapeDtypeStruct(*one) for one in outs],
            in_specs=[pl.BlockSpec(memory_space=pltpu.VMEM)] * 9,
            out_specs=[pl.BlockSpec(memory_space=pl.ANY)] * 9,
            scratch_shapes=[pltpu.SemaphoreType.DMA((9,))],
            compiler_params=pltpu.CompilerParams(vmem_limit_bytes=2**20),
        )(*res)
        return tuple(r.reshape(layers, -1, r.shape[-1]) for r in res)

    all_of, cut = P(None, None, None), P(None, "dp", None)
    return jax.shard_map(
        step,
        mesh=mesh,
        in_specs=(P(("rep", "dp"), None, None, None),) * 3 + (all_of,) * 3 + (cut,) * 6,
        out_specs=(P("rep", None, None),) * 3 + (P("rep", "dp", None),) * 6,
        check_vma=False,
    )
```

```python
import functools
import heapq
import math

import jax
import jax.numpy as jnp
from jax import lax
from jax.experimental import pallas as pl
from jax.experimental.pallas import tpu as pltpu
from jax.sharding import PartitionSpec as P

F32, BF16 = jnp.float32, jnp.bfloat16
MESH = pl.DeviceIdType.MESH
SIGN = (1, -1)
LAG_NS = 16000


def next_device(me, side, axis, d):
    at = (me // side, me % side)
    moved = lax.rem(at[axis] + SIGN[d] + side, side)
    return moved * side + at[1] if axis == 0 else at[0] * side + moved


def meet(me, side):
    barrier = pltpu.get_barrier_semaphore()
    for axis in range(2):
        for d in range(2):
            pl.semaphore_signal(barrier, inc=1, device_id={"dp": next_device(me, side, axis, d)}, device_id_type=MESH)
    pl.semaphore_wait(barrier, 4)


def block_of(me, side, c, r1, r2):
    at = (me // side, me % side)
    q1, q2 = lax.rem(at[1 - c] + r1, side), lax.rem(at[c] + r2, side)
    return q2 * side + q1 if c == 0 else q1 * side + q2


def gather_order(side, part):
    free = {(a, d): 0.0 for a in range(2) for d in range(2)}
    events, start, order, count = [], [], [], 0

    def enqueue(now, link, piece, d, first):
        nonlocal count
        c, r1, r2, h, p = piece
        free[link] = max(free[link], now) + 2.0
        there = (c, (r1 - SIGN[d]) % side, r2, h, p) if first else (c, r1, (r2 - SIGN[d]) % side, h, p)
        count += 1
        heapq.heappush(events, (free[link] + 1.0, count, there, link))

    def sends(piece, link):
        c, r1, r2, h, p = piece
        axes = (1, 0) if c == 0 else (0, 1)
        out = []
        if r1 == 0 and r2 == 0:
            out += [(axes[0], d, True) for d in range(2)]
        if r2 == 0:
            if r1 != 0 and r1 != 2 and link[1] == h:
                out.append((axes[0], h, True))
            out += [(axes[1], d, False) for d in range(2)]
        elif r2 != 2 and link[1] == h:
            out.append((axes[1], h, False))
        return out

    now = 0.0
    for h in range(2):
        for c in range(2):
            piece = (c, 0, 0, h, part)
            todo = sends(piece, None)
            start.append((piece, todo))
            for a, d, first in todo:
                enqueue(now, (a, d), piece, d, first)
            now += 0.1
    while events:
        now, _, piece, link = heapq.heappop(events)
        todo = sends(piece, link)
        order.append((piece, todo))
        for a, d, first in todo:
            enqueue(now, (a, d), piece, d, first)
    return start, order


def columns(shape):
    return 384 if shape[-1] % 384 == 0 else 128


def loop(shape, body, carry=0):
    width = columns(shape)

    def step(i, carry):
        return body(pl.ds(pl.multiple_of(i * width, width), width), carry)

    return lax.fori_loop(0, shape[-1] // width, step, carry)


def squares(x):
    total = None
    for i in range(0, x.shape[0], 8):
        for j in range(0, x.shape[1], 128):
            one = x[i : i + 8, j : j + 128]
            total = one * one if total is None else total + one * one
    return total


def kernel(n, side, count, ga, gb, gd, wa, wb, wd, ma, mb, md, va, vb, vd,
           oa, ob, mine_down, oma, omb, omd, ova, ovb, ovd,
           od, fwd_big, fwd_small, own_big, own_small, acc_big, acc_small, w_big, w_small, part,
           load_sem, send_big, send_small, recv, part_send, part_recv):
    me = lax.axis_index("dp")
    at = (me // side, me % side)

    def block(c, q1, q2):
        return q1 * side + q2 if c == 0 else q2 * side + q1

    def neighbour(axis, d):
        return next_device(me, side, axis, d)

    def near(p, steps):
        return lax.rem(p + steps + side, side)

    g_big, out_big = (ga, gb), (oa, ob)

    loads = {}

    def load(key, index, src, dst):
        copy = pltpu.make_async_copy(src, dst, load_sem.at[index])
        copy.start()
        loads[key] = copy

    def rows(ref, c, q1):
        return ref.at[c, q1] if c == 0 else ref.at[c, :, q1]

    meet(me, side)

    @pl.when(lax.rem(lax.axis_index("rep"), 2) == 0)
    def _():
        pl.delay(LAG_NS)

    def slot(c, d, p, s):
        return out_big[d].at[c * n + s] if p == 0 else od.at[c * n + s, d]

    def send(src, dst, axis, d, p, sem):
        sems = send_big if p == 0 else send_small
        link = 2 * axis + d
        pltpu.make_async_remote_copy(
            src_ref=src, dst_ref=dst, send_sem=sems.at[link if p == 0 else axis], recv_sem=sem,
            device_id={"dp": neighbour(axis, d)}, device_id_type=MESH).start()

    def arrived(ref, sem):
        pltpu.make_async_copy(ref, ref, sem).wait()

    def to_slot(src, c, d, axis, p, s):
        send(src, slot(c, d, p, s), axis, d, p, recv.at[c, d, p, s])

    def wait_slot(c, d, p, s):
        arrived(slot(c, d, p, s), recv.at[c, d, p, s])

    def term_ref(c, h, p, q1, q2):
        i, j = (q1, q2) if c == 0 else (q2, q1)
        return g_big[h].at[c, i, j] if p == 0 else gd.at[c, i, j, h]

    ks = (2, 1, -1, 0)

    def step1(c, d, k):
        for p in range(2):
            to_slot(term_ref(c, d, p, near(at[c], 2), near(at[1 - c], ks[k])), c, d, c, p, k)

    def step2(c, d, k):
        for p in range(2):
            to_slot(term_ref(c, 1 - d, p, near(at[c], SIGN[d]), near(at[1 - c], ks[k])), c, d, c, p, 4 + k)

    for k in range(4):
        for d in range(2):
            for c in range(2):
                step1(c, d, k)
    for k in range(2):
        for d in range(2):
            for c in range(2):
                step2(c, d, k)

    index = 0
    for d in range(2):
        for c in range(2):
            q1 = near(at[c], SIGN[d])
            load(("fwd", c, d, 0), index, rows(g_big[d], c, q1), fwd_big.at[c, d])
            load(("fwd", c, d, 1), index + 1, (gd.at[c, q1, :, d] if c == 0 else gd.at[c, :, q1, d]), fwd_small.at[c, d])
            index += 2
    for h in range(2):
        for c in range(2):
            load(("own", c, h, 0), index, rows(g_big[h], c, at[c]), own_big.at[c, h])
            load(("own", c, h, 1), index + 1, (gd.at[c, at[c], :, h] if c == 0 else gd.at[c, :, at[c], h]), own_small.at[c, h])
            index += 2

    own = (own_big, own_small)
    fwd = (fwd_big, fwd_small)
    acc = (acc_big, acc_small)
    shapes = (own_big.shape[-2:], own_small.shape[-2:])

    for copy in list(loads.values())[: 8]:
        copy.wait()

    def add_fwd(c, d, p, s, src):
        dst = slot(c, d, p, s)

        def body(cols, _):
            dst[:, cols] = (dst[:, cols].astype(F32) + src[:, cols].astype(F32)).astype(BF16)
            return 0

        loop(shapes[p], body)

    for k in range(4):
        for d in range(2):
            for c in range(2):
                for p in range(2):
                    wait_slot(c, d, p, k)
                    add_fwd(c, d, p, k, fwd[p].at[c, d, near(at[1 - c], ks[k])])
                    to_slot(slot(c, d, p, k), c, d, c, p, 8 + k)
                if k < 2:
                    step2(c, d, k + 2)

    for copy in list(loads.values())[8:]:
        copy.wait()

    updates = {}
    for h, (m, v, w, om, ov) in enumerate(((ma, va, wa, oma, ova), (mb, vb, wb, omb, ovb))):
        load(("m", h, 0), index, m, om)
        load(("v", h, 0), index + 1, v, ov)
        load(("w", h, 0), index + 2, w.at[:, me], w_big.at[h])
        index += 3
    load(("m", 1), index, md, omd)
    load(("v", 1), index + 1, vd, ovd)
    load(("w", 1), index + 2, wd.at[:, me], w_small)

    for k in range(4):
        for h in range(2):
            for c in range(2):
                q2 = near(at[1 - c], ks[k])
                for p in range(2):
                    wait_slot(c, h, p, 8 + k)
                    wait_slot(c, 1 - h, p, 4 + k)
                    mine, one, two = own[p].at[c, h, q2], slot(c, h, p, 8 + k), slot(c, 1 - h, p, 4 + k)
                    dst = mine if k < 3 else acc[p].at[c, h]

                    def body(cols, _, mine=mine, one=one, two=two, dst=dst):
                        x = mine[:, cols].astype(F32) + one[:, cols].astype(F32) + two[:, cols].astype(F32)
                        dst[:, cols] = x.astype(dst.dtype)
                        return 0

                    loop(shapes[p], body)
                    if k == 0:
                        to_slot(mine, c, h, 1 - c, p, 12)
                    if (k == 1 and h == 1) or (k == 2 and h == 0):
                        to_slot(mine, c, 1 - h, 1 - c, p, 13)

    for p in range(2):
        for d in range(2):
            for c in range(2):
                wait_slot(c, d, p, 12)
                add_fwd(c, d, p, 12, own[p].at[c, d, near(at[1 - c], SIGN[d])])
                to_slot(slot(c, d, p, 12), c, d, 1 - c, p, 14)

    total = jnp.zeros((8, 128), F32)
    for p in range(2):
        for h in range(2):
            for c in range(2):
                wait_slot(c, h, p, 14)
                wait_slot(c, 1 - h, p, 13)
                mine, one, two = acc[p].at[c, h], slot(c, h, p, 14), slot(c, 1 - h, p, 13)

                def body(cols, total, mine=mine, one=one, two=two):
                    x = mine[:, cols] + one[:, cols].astype(F32) + two[:, cols].astype(F32)
                    x = x.astype(BF16).astype(F32)
                    mine[:, cols] = x
                    return total + squares(x)

                total = loop(shapes[p], body, total)

    def wait_sends(parts):
        many = n - 1
        if 0 in parts:
            for link in range(4):
                ref = oa.at[pl.ds(0, many)]
                pltpu.make_async_copy(ref, ref, send_big.at[link]).wait()
        if 1 in parts:
            for axis in range(2):
                ref = od.at[pl.ds(0, many)]
                pltpu.make_async_copy(ref, ref, send_small.at[axis]).wait()

    wait_sends((0, 1))

    part[me] = jnp.sum(total, axis=0, keepdims=True)
    copies = []
    def far(i):
        return sum(min(k, side - k) for k in (i // side, i % side))

    def shifted(i, sign):
        return near(at[0], sign * (i // side)) * side + near(at[1], sign * (i % side))

    for i in sorted(range(1, n), key=far, reverse=True):
        to = shifted(i, 1)
        copy = pltpu.make_async_remote_copy(
            src_ref=part.at[me], dst_ref=part.at[me], send_sem=part_send.at[i - 1], recv_sem=part_recv.at[i - 1],
            device_id={"dp": to}, device_id_type=MESH)
        copy.start()
        copies.append(copy)
    for copy in list(loads.values())[16:]:
        copy.wait()
    for i in range(1, n):
        back = shifted(i, -1)
        arrived(part.at[back], part_recv.at[i - 1])
    total = part[0]
    for i in range(1, n):
        total = total + part[i]
    total = jnp.sum(total, keepdims=True)
    factor = jnp.minimum(1.0, 0.5 * lax.rsqrt(total / count + 1e-30))

    oms, ovs = (oma, omb), (ova, ovb)
    start, order = gather_order(side, 0)

    def gathered(piece):
        c, r1, r2, h, _ = piece
        b = block_of(me, side, c, r1, r2)
        return out_big[h].at[c * n + b], recv.at[c, h, 0, b]

    def pass_on(piece, todo):
        ref, sem = gathered(piece)
        for a, d, _ in todo:
            send(ref, ref, a, d, 0, sem)

    def take_step(g, m, v, w, out):
        def body(cols, _):
            x = g[:, cols] * factor
            m1 = 0.9 * m[:, cols] + 0.1 * x
            v1 = 0.95 * v[:, cols] + 0.05 * x * x
            m[:, cols] = m1
            v[:, cols] = v1
            w1 = w[:, cols].astype(F32)
            out[:, cols] = (w1 - 0.02 * (m1 * lax.rsqrt(v1 + 1e-8) + 0.1 * w1)).astype(BF16)
            return 0

        loop(g.shape, body)

    for piece, todo in start:
        c, _, _, h, _ = piece
        take_step(acc_big.at[c, h], oms[h].at[c], ovs[h].at[c], w_big.at[h, c], gathered(piece)[0])
        pass_on(piece, todo)
    for c in range(2):
        for h in range(2):
            take_step(acc_small.at[c, h], omd.at[c, h], ovd.at[c, h], w_small.at[c, h], mine_down.at[c, h])
    for piece, todo in order:
        arrived(*gathered(piece))
        pass_on(piece, todo)
    wait_sends((0,))
    for copy in copies:
        copy.wait_send()


def gather_down(n, side, mine, after, out, send_sem, recv):
    me = lax.axis_index("dp")
    meet(me, side)
    start, order = gather_order(side, 1)

    def gathered(piece):
        c, r1, r2, h, _ = piece
        b = block_of(me, side, c, r1, r2)
        return out.at[c * n + b, h], recv.at[c, h, b]

    def pass_on(piece, todo, src=None):
        ref, sem = gathered(piece)
        for a, d, _ in todo:
            pltpu.make_async_remote_copy(
                src_ref=ref if src is None else src, dst_ref=ref, send_sem=send_sem.at[a], recv_sem=sem,
                device_id={"dp": next_device(me, side, a, d)}, device_id_type=MESH).start()

    for piece, todo in start:
        pass_on(piece, todo, mine.at[piece[0], piece[3]])
    for piece, _ in start:
        gathered(piece)[0][...] = mine[piece[0], piece[3]]
    for piece, todo in order:
        ref, sem = gathered(piece)
        pltpu.make_async_copy(ref, ref, sem).wait()
        pass_on(piece, todo)
    for axis in range(2):
        ref = out.at[pl.ds(0, n - 1)]
        pltpu.make_async_copy(ref, ref, send_sem.at[axis]).wait()


def write_out(many, *refs):
    copies = [pltpu.make_async_copy(refs[i], refs[many + i], refs[-1].at[i]) for i in range(many)]
    for copy in copies:
        copy.start()
    for ref in refs[2 * many : -1]:
        ref[...] = jnp.zeros(ref.shape, F32)
    for copy in copies:
        copy.wait()


def solution(mesh):
    n = mesh.shape["dp"]
    side = math.isqrt(n)

    def step(*arrays):
        terms, weights, m, v = (arrays[i : i + 3] for i in (0, 3, 6, 9))
        layers, block_rows, wide = m[0].shape
        down_rows, narrow = m[2].shape[1] // 2, m[2].shape[2]
        big, small = (block_rows, wide), (down_rows, narrow)
        ins = [terms[0].reshape(layers, side, side, *big), terms[1].reshape(layers, side, side, *big),
               terms[2].reshape(layers, side, side, 2, *small),
               weights[0].reshape(layers, n, *big), weights[1].reshape(layers, n, *big), weights[2].reshape(layers, n, 2, *small)]
        for three in (m, v):
            ins += [three[0], three[1], three[2].reshape(layers, 2, *small)]
        outs = [((layers * n, *big), BF16)] * 2 + [((layers * n, 2, *small), BF16)]
        outs += ([((layers, *big), F32)] * 2 + [((layers, 2, *small), F32)]) * 2
        count = n * sum(one.size for one in m)
        res = pl.pallas_call(
            functools.partial(kernel, n, side, count),
            out_shape=[pltpu.VMEM(*one) for one in (*outs[:2], ((layers, 2, *small), BF16), *outs[3:])],
            in_specs=[pl.BlockSpec(memory_space=pl.ANY)] * 12,
            out_specs=[pl.BlockSpec(memory_space=pltpu.VMEM)] * 9,
            scratch_shapes=[
                pltpu.VMEM(*outs[2]),
                pltpu.VMEM((layers, 2, side, *big), BF16),
                pltpu.VMEM((layers, 2, side, *small), BF16),
                pltpu.VMEM((layers, 2, side, *big), BF16),
                pltpu.VMEM((layers, 2, side, *small), BF16),
                pltpu.VMEM((layers, 2, *big), F32),
                pltpu.VMEM((layers, 2, *small), F32),
                pltpu.VMEM((2, layers, *big), BF16),
                pltpu.VMEM((layers, 2, *small), BF16),
                pltpu.VMEM((n, 1, 128), F32),
                pltpu.SemaphoreType.DMA((25,)),
                pltpu.SemaphoreType.DMA((4,)),
                pltpu.SemaphoreType.DMA((2,)),
                pltpu.SemaphoreType.DMA((layers, 2, 2, n)),
                pltpu.SemaphoreType.DMA((n - 1,)),
                pltpu.SemaphoreType.DMA((n - 1,)),
            ],
            compiler_params=pltpu.CompilerParams(collective_id=0, has_side_effects=True, vmem_limit_bytes=32 * 2**20),
        )(*ins)
        def write(arrays, more):
            return pl.pallas_call(
                functools.partial(write_out, len(arrays)),
                out_shape=[*(jax.ShapeDtypeStruct(one.shape, one.dtype) for one in arrays), *[jax.ShapeDtypeStruct((8, 128), F32)] * more],
                in_specs=[pl.BlockSpec(memory_space=pltpu.VMEM)] * len(arrays),
                out_specs=[pl.BlockSpec(memory_space=pl.ANY)] * len(arrays) + [pl.BlockSpec(memory_space=pltpu.VMEM)] * more,
                scratch_shapes=[pltpu.SemaphoreType.DMA((len(arrays),))],
                compiler_params=pltpu.CompilerParams(vmem_limit_bytes=2**20),
            )(*arrays)

        written = write([*res[:2], *res[3:]], 1)
        down = pl.pallas_call(
            functools.partial(gather_down, n, side),
            out_shape=pltpu.VMEM(*outs[2]),
            in_specs=[pl.BlockSpec(memory_space=pltpu.VMEM), pl.BlockSpec(memory_space=pl.ANY)],
            out_specs=pl.BlockSpec(memory_space=pltpu.VMEM),
            scratch_shapes=[pltpu.SemaphoreType.DMA((2,)), pltpu.SemaphoreType.DMA((layers, 2, n))],
            compiler_params=pltpu.CompilerParams(collective_id=1, has_side_effects=True, vmem_limit_bytes=2 * 2**20),
        )(res[2], written[-1])
        res = [*written[:2], write([down], 0)[0], *written[2:-1]]
        return tuple(r.reshape(layers, -1, r.shape[-1]) for r in res)

    all_of, cut = P(None, None, None), P(None, "dp", None)
    return jax.shard_map(
        step,
        mesh=mesh,
        in_specs=(P(("rep", "dp"), None, None, None),) * 3 + (all_of,) * 3 + (cut,) * 6,
        out_specs=(P("rep", None, None),) * 3 + (P("rep", "dp", None),) * 6,
        check_vma=False,
    )
```

```python
import functools
import heapq
import math

import jax
import jax.numpy as jnp
from jax import lax
from jax.experimental import pallas as pl
from jax.experimental.pallas import tpu as pltpu
from jax.sharding import PartitionSpec as P

F32, BF16 = jnp.float32, jnp.bfloat16
MESH = pl.DeviceIdType.MESH
SIGN = (1, -1)
LAG_NS = 16000


def next_device(me, side, axis, d):
    at = (me // side, me % side)
    moved = lax.rem(at[axis] + SIGN[d] + side, side)
    return moved * side + at[1] if axis == 0 else at[0] * side + moved


def meet(me, side):
    barrier = pltpu.get_barrier_semaphore()
    for axis in range(2):
        for d in range(2):
            pl.semaphore_signal(barrier, inc=1, device_id={"dp": next_device(me, side, axis, d)}, device_id_type=MESH)
    pl.semaphore_wait(barrier, 4)


def block_of(me, side, c, r1, r2):
    at = (me // side, me % side)
    q1, q2 = lax.rem(at[1 - c] + r1, side), lax.rem(at[c] + r2, side)
    return q2 * side + q1 if c == 0 else q1 * side + q2


def gather_order(side, part):
    free = {(a, d): 0.0 for a in range(2) for d in range(2)}
    events, start, order, count = [], [], [], 0

    def enqueue(now, link, piece, d, first):
        nonlocal count
        c, r1, r2, h, p = piece
        free[link] = max(free[link], now) + 2.0
        there = (c, (r1 - SIGN[d]) % side, r2, h, p) if first else (c, r1, (r2 - SIGN[d]) % side, h, p)
        count += 1
        heapq.heappush(events, (free[link] + 1.0, count, there, link))

    def sends(piece, link):
        c, r1, r2, h, p = piece
        axes = (1, 0) if c == 0 else (0, 1)
        out = []
        if r1 == 0 and r2 == 0:
            out += [(axes[0], d, True) for d in range(2)]
        if r2 == 0:
            if r1 != 0 and r1 != 2 and link[1] == h:
                out.append((axes[0], h, True))
            out += [(axes[1], d, False) for d in range(2)]
        elif r2 != 2 and link[1] == h:
            out.append((axes[1], h, False))
        return out

    now = 0.0
    for h in range(2):
        for c in range(2):
            start.append(((c, 0, 0, h, part), sends((c, 0, 0, h, part), None)))
    if part == 1:
        start = [(piece, [one for one in todo if (one[1] == piece[3]) == now]) for now in (True, False) for piece, todo in start]
    now = 0.0
    for piece, todo in start:
        for a, d, first in todo:
            enqueue(now, (a, d), piece, d, first)
        now += 0.1
    while events:
        now, _, piece, link = heapq.heappop(events)
        todo = sends(piece, link)
        order.append((piece, todo))
        for a, d, first in todo:
            enqueue(now, (a, d), piece, d, first)
    return start, order


def columns(shape):
    return 384 if shape[-1] % 384 == 0 else 128


def loop(shape, body, carry=0):
    width = columns(shape)

    def step(i, carry):
        return body(pl.ds(pl.multiple_of(i * width, width), width), carry)

    return lax.fori_loop(0, shape[-1] // width, step, carry)


def squares(x):
    total = None
    for i in range(0, x.shape[0], 8):
        for j in range(0, x.shape[1], 128):
            one = x[i : i + 8, j : j + 128]
            total = one * one if total is None else total + one * one
    return total


def kernel(n, side, count, ga, gb, gd, wa, wb, wd, ma, mb, md, va, vb, vd,
           oa, ob, mine_down, oma, omb, omd, ova, ovb, ovd,
           od, fwd_big, fwd_small, own_big, own_small, acc_big, acc_small, w_big, w_small, part,
           load_sem, send_big, send_small, recv, part_send, part_recv):
    me = lax.axis_index("dp")
    at = (me // side, me % side)

    def block(c, q1, q2):
        return q1 * side + q2 if c == 0 else q2 * side + q1

    def neighbour(axis, d):
        return next_device(me, side, axis, d)

    def near(p, steps):
        return lax.rem(p + steps + side, side)

    g_big, out_big = (ga, gb), (oa, ob)

    loads = {}

    def load(key, index, src, dst):
        copy = pltpu.make_async_copy(src, dst, load_sem.at[index])
        copy.start()
        loads[key] = copy

    def rows(ref, c, q1):
        return ref.at[c, q1] if c == 0 else ref.at[c, :, q1]

    meet(me, side)

    @pl.when(lax.rem(lax.axis_index("rep"), 2) == 0)
    def _():
        pl.delay(LAG_NS)

    def slot(c, d, p, s):
        return out_big[d].at[c * n + s] if p == 0 else od.at[c * n + s, d]

    def send(src, dst, axis, d, p, sem):
        sems = send_big if p == 0 else send_small
        link = 2 * axis + d
        pltpu.make_async_remote_copy(
            src_ref=src, dst_ref=dst, send_sem=sems.at[link if p == 0 else axis], recv_sem=sem,
            device_id={"dp": neighbour(axis, d)}, device_id_type=MESH).start()

    def arrived(ref, sem):
        pltpu.make_async_copy(ref, ref, sem).wait()

    def to_slot(src, c, d, axis, p, s):
        send(src, slot(c, d, p, s), axis, d, p, recv.at[c, d, p, s])

    def wait_slot(c, d, p, s):
        arrived(slot(c, d, p, s), recv.at[c, d, p, s])

    def term_ref(c, h, p, q1, q2):
        i, j = (q1, q2) if c == 0 else (q2, q1)
        return g_big[h].at[c, i, j] if p == 0 else gd.at[c, i, j, h]

    ks = (2, 1, -1, 0)

    def step1(c, d, k):
        for p in range(2):
            to_slot(term_ref(c, d, p, near(at[c], 2), near(at[1 - c], ks[k])), c, d, c, p, k)

    def step2(c, d, k):
        for p in range(2):
            to_slot(term_ref(c, 1 - d, p, near(at[c], SIGN[d]), near(at[1 - c], ks[k])), c, d, c, p, 4 + k)

    for k in range(4):
        for d in range(2):
            for c in range(2):
                step1(c, d, k)
    for k in range(2):
        for d in range(2):
            for c in range(2):
                step2(c, d, k)

    index = 0
    for d in range(2):
        for c in range(2):
            q1 = near(at[c], SIGN[d])
            load(("fwd", c, d, 0), index, rows(g_big[d], c, q1), fwd_big.at[c, d])
            load(("fwd", c, d, 1), index + 1, (gd.at[c, q1, :, d] if c == 0 else gd.at[c, :, q1, d]), fwd_small.at[c, d])
            index += 2
    for h in range(2):
        for c in range(2):
            load(("own", c, h, 0), index, rows(g_big[h], c, at[c]), own_big.at[c, h])
            load(("own", c, h, 1), index + 1, (gd.at[c, at[c], :, h] if c == 0 else gd.at[c, :, at[c], h]), own_small.at[c, h])
            index += 2

    own = (own_big, own_small)
    fwd = (fwd_big, fwd_small)
    acc = (acc_big, acc_small)
    shapes = (own_big.shape[-2:], own_small.shape[-2:])

    for copy in list(loads.values())[: 8]:
        copy.wait()

    def add_fwd(c, d, p, s, src):
        dst = slot(c, d, p, s)

        def body(cols, _):
            dst[:, cols] = (dst[:, cols].astype(F32) + src[:, cols].astype(F32)).astype(BF16)
            return 0

        loop(shapes[p], body)

    for k in range(4):
        for d in range(2):
            for c in range(2):
                for p in range(2):
                    wait_slot(c, d, p, k)
                    add_fwd(c, d, p, k, fwd[p].at[c, d, near(at[1 - c], ks[k])])
                    to_slot(slot(c, d, p, k), c, d, c, p, 8 + k)
                if k < 2:
                    step2(c, d, k + 2)

    for copy in list(loads.values())[8:]:
        copy.wait()

    updates = {}
    for h, (m, v, w, om, ov) in enumerate(((ma, va, wa, oma, ova), (mb, vb, wb, omb, ovb))):
        load(("m", h, 0), index, m, om)
        load(("v", h, 0), index + 1, v, ov)
        load(("w", h, 0), index + 2, w.at[:, me], w_big.at[h])
        index += 3
    load(("m", 1), index, md, omd)
    load(("v", 1), index + 1, vd, ovd)
    load(("w", 1), index + 2, wd.at[:, me], w_small)

    for k in range(4):
        for h in range(2):
            for c in range(2):
                q2 = near(at[1 - c], ks[k])
                for p in range(2):
                    wait_slot(c, h, p, 8 + k)
                    wait_slot(c, 1 - h, p, 4 + k)
                    mine, one, two = own[p].at[c, h, q2], slot(c, h, p, 8 + k), slot(c, 1 - h, p, 4 + k)
                    dst = mine if k < 3 else acc[p].at[c, h]

                    def body(cols, _, mine=mine, one=one, two=two, dst=dst):
                        x = mine[:, cols].astype(F32) + one[:, cols].astype(F32) + two[:, cols].astype(F32)
                        dst[:, cols] = x.astype(dst.dtype)
                        return 0

                    loop(shapes[p], body)
                    if k == 0:
                        to_slot(mine, c, h, 1 - c, p, 12)
                    if (k == 1 and h == 1) or (k == 2 and h == 0):
                        to_slot(mine, c, 1 - h, 1 - c, p, 13)

    for p in range(2):
        for d in range(2):
            for c in range(2):
                wait_slot(c, d, p, 12)
                add_fwd(c, d, p, 12, own[p].at[c, d, near(at[1 - c], SIGN[d])])
                to_slot(slot(c, d, p, 12), c, d, 1 - c, p, 14)

    total = jnp.zeros((8, 128), F32)
    for p in range(2):
        for h in range(2):
            for c in range(2):
                wait_slot(c, h, p, 14)
                wait_slot(c, 1 - h, p, 13)
                mine, one, two = acc[p].at[c, h], slot(c, h, p, 14), slot(c, 1 - h, p, 13)

                def body(cols, total, mine=mine, one=one, two=two):
                    x = mine[:, cols] + one[:, cols].astype(F32) + two[:, cols].astype(F32)
                    x = x.astype(BF16).astype(F32)
                    mine[:, cols] = x
                    return total + squares(x)

                total = loop(shapes[p], body, total)

    def wait_sends(parts):
        many = n - 1
        if 0 in parts:
            for link in range(4):
                ref = oa.at[pl.ds(0, many)]
                pltpu.make_async_copy(ref, ref, send_big.at[link]).wait()
        if 1 in parts:
            for axis in range(2):
                ref = od.at[pl.ds(0, many)]
                pltpu.make_async_copy(ref, ref, send_small.at[axis]).wait()

    wait_sends((0, 1))

    part[me] = jnp.sum(total, axis=0, keepdims=True)
    copies = []
    def far(i):
        return sum(min(k, side - k) for k in (i // side, i % side))

    def shifted(i, sign):
        return near(at[0], sign * (i // side)) * side + near(at[1], sign * (i % side))

    for i in sorted(range(1, n), key=far, reverse=True):
        to = shifted(i, 1)
        copy = pltpu.make_async_remote_copy(
            src_ref=part.at[me], dst_ref=part.at[me], send_sem=part_send.at[i - 1], recv_sem=part_recv.at[i - 1],
            device_id={"dp": to}, device_id_type=MESH)
        copy.start()
        copies.append(copy)
    for copy in list(loads.values())[16:]:
        copy.wait()
    for i in range(1, n):
        back = shifted(i, -1)
        arrived(part.at[back], part_recv.at[i - 1])
    total = part[0]
    for i in range(1, n):
        total = total + part[i]
    total = jnp.sum(total, keepdims=True)
    factor = jnp.minimum(1.0, 0.5 * lax.rsqrt(total / count + 1e-30))

    oms, ovs = (oma, omb), (ova, ovb)
    start, order = gather_order(side, 0)

    def gathered(piece):
        c, r1, r2, h, _ = piece
        b = block_of(me, side, c, r1, r2)
        return out_big[h].at[c * n + b], recv.at[c, h, 0, b]

    def pass_on(piece, todo):
        ref, sem = gathered(piece)
        for a, d, _ in todo:
            send(ref, ref, a, d, 0, sem)

    def take_step(g, m, v, w, out):
        def body(cols, _):
            x = g[:, cols] * factor
            m1 = 0.9 * m[:, cols] + 0.1 * x
            v1 = 0.95 * v[:, cols] + 0.05 * x * x
            m[:, cols] = m1
            v[:, cols] = v1
            w1 = w[:, cols].astype(F32)
            out[:, cols] = (w1 - 0.02 * (m1 * lax.rsqrt(v1 + 1e-8) + 0.1 * w1)).astype(BF16)
            return 0

        loop(g.shape, body)

    for piece, todo in start:
        c, _, _, h, _ = piece
        take_step(acc_big.at[c, h], oms[h].at[c], ovs[h].at[c], w_big.at[h, c], gathered(piece)[0])
        pass_on(piece, todo)
    for c in range(2):
        for h in range(2):
            take_step(acc_small.at[c, h], omd.at[c, h], ovd.at[c, h], w_small.at[c, h], mine_down.at[c, h])
    for piece, todo in order:
        arrived(*gathered(piece))
        pass_on(piece, todo)
    wait_sends((0,))
    for copy in copies:
        copy.wait_send()


def gather_down(n, side, mine, after, out, send_sem, recv):
    me = lax.axis_index("dp")
    meet(me, side)
    start, order = gather_order(side, 1)

    def gathered(piece):
        c, r1, r2, h, _ = piece
        b = block_of(me, side, c, r1, r2)
        return out.at[c * n + b, h], recv.at[c, h, b]

    def pass_on(piece, todo, src=None):
        ref, sem = gathered(piece)
        for a, d, _ in todo:
            pltpu.make_async_remote_copy(
                src_ref=ref if src is None else src, dst_ref=ref, send_sem=send_sem.at[a], recv_sem=sem,
                device_id={"dp": next_device(me, side, a, d)}, device_id_type=MESH).start()

    for piece, todo in start:
        pass_on(piece, todo, mine.at[piece[0], piece[3]])
    for piece in dict.fromkeys(piece for piece, _ in start):
        gathered(piece)[0][...] = mine[piece[0], piece[3]]
    for piece, todo in order:
        ref, sem = gathered(piece)
        pltpu.make_async_copy(ref, ref, sem).wait()
        pass_on(piece, todo)
    for axis in range(2):
        ref = out.at[pl.ds(0, n - 1)]
        pltpu.make_async_copy(ref, ref, send_sem.at[axis]).wait()


def write_out(many, *refs):
    copies = [pltpu.make_async_copy(refs[i], refs[many + i], refs[-1].at[i]) for i in range(many)]
    for copy in copies:
        copy.start()
    for ref in refs[2 * many : -1]:
        ref[...] = jnp.zeros(ref.shape, F32)
    for copy in copies:
        copy.wait()


def solution(mesh):
    n = mesh.shape["dp"]
    side = math.isqrt(n)

    def step(*arrays):
        terms, weights, m, v = (arrays[i : i + 3] for i in (0, 3, 6, 9))
        layers, block_rows, wide = m[0].shape
        down_rows, narrow = m[2].shape[1] // 2, m[2].shape[2]
        big, small = (block_rows, wide), (down_rows, narrow)
        ins = [terms[0].reshape(layers, side, side, *big), terms[1].reshape(layers, side, side, *big),
               terms[2].reshape(layers, side, side, 2, *small),
               weights[0].reshape(layers, n, *big), weights[1].reshape(layers, n, *big), weights[2].reshape(layers, n, 2, *small)]
        for three in (m, v):
            ins += [three[0], three[1], three[2].reshape(layers, 2, *small)]
        outs = [((layers * n, *big), BF16)] * 2 + [((layers * n, 2, *small), BF16)]
        outs += ([((layers, *big), F32)] * 2 + [((layers, 2, *small), F32)]) * 2
        count = n * sum(one.size for one in m)
        res = pl.pallas_call(
            functools.partial(kernel, n, side, count),
            out_shape=[pltpu.VMEM(*one) for one in (*outs[:2], ((layers, 2, *small), BF16), *outs[3:])],
            in_specs=[pl.BlockSpec(memory_space=pl.ANY)] * 12,
            out_specs=[pl.BlockSpec(memory_space=pltpu.VMEM)] * 9,
            scratch_shapes=[
                pltpu.VMEM(*outs[2]),
                pltpu.VMEM((layers, 2, side, *big), BF16),
                pltpu.VMEM((layers, 2, side, *small), BF16),
                pltpu.VMEM((layers, 2, side, *big), BF16),
                pltpu.VMEM((layers, 2, side, *small), BF16),
                pltpu.VMEM((layers, 2, *big), F32),
                pltpu.VMEM((layers, 2, *small), F32),
                pltpu.VMEM((2, layers, *big), BF16),
                pltpu.VMEM((layers, 2, *small), BF16),
                pltpu.VMEM((n, 1, 128), F32),
                pltpu.SemaphoreType.DMA((25,)),
                pltpu.SemaphoreType.DMA((4,)),
                pltpu.SemaphoreType.DMA((2,)),
                pltpu.SemaphoreType.DMA((layers, 2, 2, n)),
                pltpu.SemaphoreType.DMA((n - 1,)),
                pltpu.SemaphoreType.DMA((n - 1,)),
            ],
            compiler_params=pltpu.CompilerParams(collective_id=0, has_side_effects=True, vmem_limit_bytes=32 * 2**20),
        )(*ins)
        def write(arrays, more):
            return pl.pallas_call(
                functools.partial(write_out, len(arrays)),
                out_shape=[*(jax.ShapeDtypeStruct(one.shape, one.dtype) for one in arrays), *[jax.ShapeDtypeStruct((8, 128), F32)] * more],
                in_specs=[pl.BlockSpec(memory_space=pltpu.VMEM)] * len(arrays),
                out_specs=[pl.BlockSpec(memory_space=pl.ANY)] * len(arrays) + [pl.BlockSpec(memory_space=pltpu.VMEM)] * more,
                scratch_shapes=[pltpu.SemaphoreType.DMA((len(arrays),))],
                compiler_params=pltpu.CompilerParams(vmem_limit_bytes=2**20),
            )(*arrays)

        written = write([*res[:2], *res[3:]], 1)
        down = pl.pallas_call(
            functools.partial(gather_down, n, side),
            out_shape=pltpu.VMEM(*outs[2]),
            in_specs=[pl.BlockSpec(memory_space=pltpu.VMEM), pl.BlockSpec(memory_space=pl.ANY)],
            out_specs=pl.BlockSpec(memory_space=pltpu.VMEM),
            scratch_shapes=[pltpu.SemaphoreType.DMA((2,)), pltpu.SemaphoreType.DMA((layers, 2, n))],
            compiler_params=pltpu.CompilerParams(collective_id=1, has_side_effects=True, vmem_limit_bytes=2 * 2**20),
        )(res[2], written[-1])
        res = [*written[:2], write([down], 0)[0], *written[2:-1]]
        return tuple(r.reshape(layers, -1, r.shape[-1]) for r in res)

    all_of, cut = P(None, None, None), P(None, "dp", None)
    return jax.shard_map(
        step,
        mesh=mesh,
        in_specs=(P(("rep", "dp"), None, None, None),) * 3 + (all_of,) * 3 + (cut,) * 6,
        out_specs=(P("rep", None, None),) * 3 + (P("rep", "dp", None),) * 6,
        check_vma=False,
    )
```
